256 devices in a mesh: row: 8 (over y, core), col: 32 (over x, z).
Axes of the slice: x: 4, y: 4, z: 8, core: 2. Of those that a mesh axis runs over, the one named last changes fastest.
Arguments:
- normal: float32 [8, 8, 256, 2, 32, 256], P(None, 'row', None, None, 'col'), may hold values from -1.5 to 1.5
- panel_inverse: float32 [256, 256], replicated, as said below
- rhs: float32 [8, 8, 256, 512], P(None, 'row', None, 'col'), may hold values from -0.009765625 to 0.009765625
- shifts: float32 [4], replicated, may hold values from 16 to 128
Outputs:
- schur: float32 [8, 8, 256, 2, 32, 256], P(None, 'row', None, None, 'col')
- eliminated: float32 [8, 8, 256, 512], P(None, 'row', None, 'col')
- applied: float32 [8, 8, 256, 512], P(None, 'row', None, 'col')
The draws below stay inside these ranges and needn't reach their ends.
Inputs may be any that keep to these rules, and one draw needn't show every extreme that they name: `panel_inverse`: lower triangular with positive diagonal entries.
All inputs are finite; a program needn't handle non-finite values.
Results may differ from the reference program's by a relative error of at most 0.000076.
Values sent between devices are 32-bit elements; how exact they have to be, the bound alone decides.
No kernel may reach another device: no remote copies, remote signals or barrier semaphores. Data moves between devices by JAX's collectives and lax.ppermute only.
A program may use at most 64 MiB of HBM per device.

```python
import math
import jax
import jax.numpy as jnp
from jax import lax

N = 16384
NB = 256
R = 128
GROUPS = 4
BR = 8
BC = 2
K = 512
N_ROW = 8
N_COL = 32


def draw_normal(key, part):
    inner = jax.random.fold_in(key, 29)
    base = jax.random.normal(inner, (N, N), jnp.float32) * 0.25
    mirrored = (base + base.T) * 0.5 ** 0.5
    mirrored = jnp.clip(mirrored, -1.5, 1.5)
    return mirrored.reshape(BR, N_ROW, NB, BC, N_COL, NB)


def draw_panel_inverse(key, part):
    first_key, second_key = jax.random.split(jax.random.fold_in(key, 17))
    diagonal = jax.random.uniform(first_key, (NB,), jnp.float32, 0.5, 1.5)
    offdiag = jax.random.normal(second_key, (NB, NB), jnp.float32) * (0.5 / NB ** 0.5)
    return jnp.tril(offdiag, -1) + jnp.diag(diagonal)


def steps_of(rng, dims, cuts, smallest, high):
    factor_of = 1.0
    for dim, parts in cuts:
        draws = jax.random.uniform(jax.random.fold_in(jax.random.fold_in(rng, 6), dim), (parts,), jnp.float32, smallest / len(cuts), high / len(cuts))
        factor_of = factor_of * jnp.repeat(jnp.exp(draws), dims[dim] // parts).reshape((-1,) + (1,) * (len(dims) - 1 - dim))
    return factor_of


def noise(own_key, shape, width, limit, cuts=(), held_as=jnp.bfloat16):
    result = jax.random.normal(own_key, shape, jnp.float32) * width
    if len(cuts) > 0:
        result = steps_of(own_key, shape, cuts, -0.22, 0.18) * result
    return jnp.clip(result, min=-limit, max=limit).astype(held_as)


def setup_inputs(seed: int = 0) -> dict:
    streams_of = jax.random.split(jax.random.key(seed), 5)
    normal = draw_normal(jax.random.fold_in(streams_of[4], 71), 0)
    panel_inverse = draw_panel_inverse(jax.random.fold_in(streams_of[4], 71), 0)
    rhs = noise(streams_of[2], (BR, N_ROW, NB, K), 0.0016, 0.009765625, ((1, 8), (3, 32)), jnp.float32)
    shifts = jnp.clip(jnp.exp(jax.random.uniform(streams_of[3], (GROUPS,), jnp.float32, math.log(16.0), math.log(128.0))), 16.0, 128.0)
    return dict(normal=normal, panel_inverse=panel_inverse, rhs=rhs, shifts=shifts)


def reference(normal, panel_inverse, rhs, shifts):
    high = lax.Precision.HIGHEST
    matrix = normal.reshape(N, N)
    right = rhs.reshape(N, K)
    panel = jnp.dot(matrix[:, :NB], panel_inverse.T, precision=high, preferred_element_type=jnp.float32)
    updated = matrix - jnp.dot(panel, panel.T, precision=high, preferred_element_type=jnp.float32)
    first = jnp.dot(panel_inverse, right[:NB], precision=high, preferred_element_type=jnp.float32)
    reduced = right - jnp.dot(panel, first, precision=high, preferred_element_type=jnp.float32)
    reduced = jnp.concatenate([first, reduced[NB:]], axis=0)
    scales = jnp.repeat(shifts, R)
    product = jnp.dot(updated, reduced, precision=high, preferred_element_type=jnp.float32) + reduced * scales[None, :]
    schur = updated.reshape(BR, N_ROW, NB, BC, N_COL, NB)
    return schur, reduced.reshape(BR, N_ROW, NB, K), product.reshape(BR, N_ROW, NB, K)
```

```python
import functools
import jax
import jax.numpy as jnp
from jax import lax
from jax.experimental import pallas as pl
from jax.experimental.pallas import tpu as pltpu
from jax.sharding import Mesh
from jax.sharding import PartitionSpec as P


NY, NC, NX, NZ = 4, 2, 4, 8
NB = 256
CUT = 5
F32 = jnp.float32
BF16 = jnp.bfloat16
NT = (((1,), (1,)), ((), ()))
NN = (((1,), (0,)), ((), ()))


def halves(value):
    high = value.astype(BF16)
    return high, (value - high.astype(F32)).astype(BF16)


def dot3(left, right, dims):
    total = lax.dot_general(left[0], right[0], dims, preferred_element_type=F32)
    total += lax.dot_general(left[0], right[1], dims, preferred_element_type=F32)
    return total + lax.dot_general(left[1], right[0], dims, preferred_element_type=F32)


def panel_kernel(place, tile, inverse, out):
    z = place[3]
    inv = halves(inverse[...])
    for c in range(4):
        block = tile[pl.ds(c, NB, stride=4), :]
        rows = dot3(halves(block.T), inv, NT)
        for h in range(2):
            out[(2 * c + h - z + 8) % 8] = rows[64 * h : 64 * h + 64]


def block_of(refs, dx, dz, mode):
    if mode == "zx":
        if dx == 2:
            return refs[3][dz] if dz < 4 else refs[4][dz - 4]
        return refs[{0: 0, 1: 1, 3: 2}[dx]][dz]
    if dz == 4:
        return refs[7][dx] if dx < 2 else refs[8][dx - 2]
    return refs[{0: 0, 1: 1, 7: 2, 2: 3, 6: 4, 3: 5, 5: 6}[dz]][dx]


def position(place, dx, dz):
    y, c, z = place[0], place[1], place[3]
    zt = (z + dz) % 8
    return pl.multiple_of((((zt + c) % 2) * 4 + (zt // 2 - y + 4) % 4) * 64 + dx * 16, 16)


def update_kernel(place, tile, inverse, cols, p0, p1, p2, p3, p4, schur, s_high, s_low, first, shift_out,
                  ph, plo, qh, ql, fh, fl):
    x, z = place[2], place[3]
    refs = (p0, p1, p2, p3, p4)

    @pl.when(pl.program_id(0) == 0)
    def _():
        for dx in range(4):
            xt = (x + dx) % 4
            for dz in range(8):
                zt = (z + dz) % 8
                block = block_of(refs, dx, dz, "zx")
                row = pl.multiple_of((4 * (zt // 4) + xt) * NB + 64 * (zt % 4), 64)
                high, low = halves(block[:64])
                ph[pl.ds(row, 64), :] = high
                plo[pl.ds(row, 64), :] = low
                first[pl.ds(position(place, dx, dz), 16), :] = block[64:]
        for d in range(8):
            row = pl.multiple_of(((z + d) % 8) * 64, 64)
            high, low = halves(cols[d])
            qh[pl.ds(row, 64), :] = high
            ql[pl.ds(row, 64), :] = low
        value = dot3(halves(first[...]), halves(inverse[...]), NT)
        first[...] = value
        high, low = halves(value)
        fh[...] = high
        fl[...] = low

    nrow = tile.shape[0] // 4
    start = pl.multiple_of(pl.program_id(0) * nrow, nrow)
    mine = (ph[pl.ds(start, nrow), :], plo[pl.ds(start, nrow), :])
    delta = dot3(mine, (qh[...], ql[...]), NT)
    for c in range(4):
        value = tile[pl.ds(c, nrow, stride=4), :] - delta[:, 128 * c : 128 * c + 128]
        schur[pl.ds(c, nrow, stride=4), :] = value
        high, low = halves(value)
        s_high[:, 128 * c : 128 * c + 128] = high
        s_low[:, 128 * c : 128 * c + 128] = low
    shift_out[...] = dot3((fh[...], fl[...]), mine, NT)


def apply_kernel(place, first, correction, s_high, s_low, *rest):
    early = rest[:9]
    late = rest[9:14]
    kept, sent, own, ch, cl = rest[14:]
    is_top = place[0] * 2 + place[1] == 0
    for dx in range(4):
        for dz in range(8):
            row = position(place, dx, dz)
            for a in range(8):
                if a < CUT:
                    block = block_of(early, dx, dz, "xz")[a]
                else:
                    block = block_of(late, dx, dz, "zx")[a - CUT]
                value = block - correction[pl.ds(row, 16), a * NB : a * NB + NB]
                if a == 0:
                    value = jnp.where(is_top, first[pl.ds(row, 16), :], value)
                if dx == 0 and dz == 0:
                    own[a] = value
                high, low = halves(value)
                ch[pl.ds(row, 16), a * NB : a * NB + NB] = high
                cl[pl.ds(row, 16), a * NB : a * NB + NB] = low
    right = (s_high[...], s_low[...])
    kept[...] = dot3((ch[:256], cl[:256]), right, NN)
    sent[...] = dot3((ch[256:], cl[256:]), right, NN)


def finish_kernel(place, shifts, own, r0, r1, r2, r3, out):
    x = place[2]
    scale = shifts[x]
    for dx, ref in enumerate((r0, r1, r2, r3)):
        for b in range(2):
            a = 4 * b + (x - dx + 4) % 4
            out[a] = ref[:, b * NB : b * NB + NB] + own[a] * scale


def vmem():
    return pl.BlockSpec(memory_space=pltpu.VMEM)


def smem():
    return pl.BlockSpec(memory_space=pltpu.SMEM)


def step(array, axis, by):
    size = lax.axis_size(axis)
    return lax.ppermute(array, axis, [(i, (i + by) % size) for i in range(size)])


def ring_z(block):
    got = {0: block, 1: step(block, "z", -1), 7: step(block, "z", 1)}
    got[2] = step(got[1], "z", -1)
    got[6] = step(got[7], "z", 1)
    got[3] = step(got[2], "z", -1)
    got[5] = step(got[6], "z", 1)
    return got


def z_then_x(block):
    got = ring_z(block)
    got[4] = step(got[3], "z", -1)
    plane = jnp.stack([got[d] for d in range(8)])
    right = step(plane, "x", -1)
    left = step(plane, "x", 1)
    return plane, right, left, step(right[:4], "x", -1), step(left[4:], "x", 1)


def x_then_z(block):
    line = jnp.stack([block, step(block, "x", -1), step(block, "x", 2), step(block, "x", 1)])
    got = ring_z(line)
    far = step(got[3][:2], "z", -1), step(got[5][2:], "z", 1)
    return (got[0], got[1], got[7], got[2], got[6], got[3], got[5]) + far


def index(y, c, x, z):
    return ((y * NC + c) * NX + x) * NZ + z


def to_everyone_in_row(array, place):
    copies = [lax.ppermute(array, ("y", "c"), [(0, 2 * r)]) for r in (1, 2, 3)]
    array = jnp.where(place[0] == 0, array, copies[0] + copies[1] + copies[2])
    other = lax.ppermute(array, "c", [(0, 1)])
    return jnp.where(place[1] == 0, array, other)


def shards(normal, panel_inverse, rhs, shifts):
    axes = ("y", "c", "x", "z")
    place = jnp.stack([lax.axis_index(axis) for axis in axes]).astype(jnp.int32)
    tile = normal.reshape(8192, 128)
    right = jnp.transpose(rhs.reshape(8, NB, 16), (0, 2, 1))
    top = to_everyone_in_row(right[0], place)
    early = x_then_z(right[:CUT])
    late = z_then_x(right[CUT:])

    cols = pl.pallas_call(
        panel_kernel,
        grid=(1,),
        in_specs=[smem(), pl.BlockSpec((1024, 128), lambda i: (0, 0)), pl.BlockSpec((NB, NB), lambda i: (0, 0))],
        out_specs=pl.BlockSpec((8, 64, NB), lambda i: (0, 0, 0)),
        out_shape=jax.ShapeDtypeStruct((8, 64, NB), F32),
        name="panel",
    )(place, tile, panel_inverse)
    pieces = []
    for d in range(8):
        pairs = [
            (index(0, 0, x, s), index(s // 2, s % 2, x, (s + d) % 8)) for x in range(NX) for s in range(NZ)
        ]
        pieces.append(lax.ppermute(cols[d], axes, pairs))
    piece = functools.reduce(jnp.add, pieces)
    panel = z_then_x(jnp.concatenate([piece, top], axis=0))
    cols = to_everyone_in_row(cols, place)

    nrow = 512
    steps = 2048 // nrow
    whole = lambda shape: pl.BlockSpec(shape, lambda i: (0,) * len(shape))
    schur, s_high, s_low, first, correction = pl.pallas_call(
        update_kernel,
        grid=(steps,),
        in_specs=[smem(), pl.BlockSpec((nrow * 4, 128), lambda i: (i, 0)), whole((NB, NB)), whole((8, 64, NB))]
        + [whole(part.shape) for part in panel],
        out_specs=[
            pl.BlockSpec((nrow * 4, 128), lambda i: (i, 0)),
            pl.BlockSpec((nrow, 512), lambda i: (i, 0)),
            pl.BlockSpec((nrow, 512), lambda i: (i, 0)),
            whole((512, NB)),
            pl.BlockSpec((512, nrow), lambda i: (0, i)),
        ],
        out_shape=[
            jax.ShapeDtypeStruct((8192, 128), F32),
            jax.ShapeDtypeStruct((2048, 512), BF16),
            jax.ShapeDtypeStruct((2048, 512), BF16),
            jax.ShapeDtypeStruct((512, NB), F32),
            jax.ShapeDtypeStruct((512, 2048), F32),
        ],
        scratch_shapes=[
            pltpu.VMEM((2048, NB), BF16),
            pltpu.VMEM((2048, NB), BF16),
            pltpu.VMEM((512, NB), BF16),
            pltpu.VMEM((512, NB), BF16),
            pltpu.VMEM((512, NB), BF16),
            pltpu.VMEM((512, NB), BF16),
        ],
        name="update",
    )(place, tile, panel_inverse, cols, *panel)

    kept, sent, own = pl.pallas_call(
        apply_kernel,
        in_specs=[smem()] + [vmem()] * 18,
        out_specs=[vmem()] * 3,
        out_shape=[
            jax.ShapeDtypeStruct((256, 512), F32),
            jax.ShapeDtypeStruct((256, 512), F32),
            jax.ShapeDtypeStruct((8, 16, NB), F32),
        ],
        scratch_shapes=[pltpu.VMEM((512, 2048), BF16), pltpu.VMEM((512, 2048), BF16)],
        name="apply",
    )(place, first, correction, s_high, s_low, *early, *late)

    kept = kept + lax.ppermute(sent, "c", [(0, 1), (1, 0)])
    parts = [step(kept[64 * r : 64 * r + 64], "y", r) for r in (1, 2, 3)]
    total = kept[:64] + parts[0] + parts[1] + parts[2]
    arrived = []
    for dx in range(4):
        pairs = [
            (index(p // 2, p % 2, x, z), index(z // 2, z % 2, (x + dx) % 4, p))
            for p in range(8)
            for x in range(NX)
            for z in range(NZ)
        ]
        arrived.append(lax.ppermute(total[16 * dx : 16 * dx + 16], axes, pairs))
    applied = pl.pallas_call(
        finish_kernel,
        in_specs=[smem(), smem()] + [vmem()] * 5,
        out_specs=vmem(),
        out_shape=jax.ShapeDtypeStruct((8, 16, NB), F32),
        name="finish",
    )(place, shifts, own, *arrived)

    def in_rhs_layout(array):
        return jnp.transpose(array, (0, 2, 1)).reshape(8, 1, NB, 16)

    return schur.reshape(8, 1, NB, 2, 1, NB), in_rhs_layout(own), in_rhs_layout(applied)


def solution(mesh):
    split = Mesh(mesh.devices.reshape(NY, NC, NX, NZ), ("y", "c", "x", "z"))
    row, col = ("y", "c"), ("x", "z")
    matrix = P(None, row, None, None, col, None)
    sides = P(None, row, None, col)
    return jax.shard_map(
        shards,
        mesh=split,
        in_specs=(matrix, P(), sides, P()),
        out_specs=(matrix, sides, sides),
        check_vma=False,
    )
```

```python
import jax
import jax.numpy as jnp
from jax import lax
from jax.experimental import pallas as pl
from jax.experimental.pallas import tpu as pltpu
from jax.sharding import Mesh
from jax.sharding import PartitionSpec as P


NY, NC, NX, NZ = 4, 2, 4, 8
AXES = ("y", "c", "x", "z")
NB = 256
CUT = 4
F32 = jnp.float32
BF16 = jnp.bfloat16
NT = (((1,), (1,)), ((), ()))
NN = (((1,), (0,)), ((), ()))


def halves(value):
    high = value.astype(BF16)
    return high, (value - high.astype(F32)).astype(BF16)


def dot3(left, right, dims):
    total = lax.dot_general(left[0], right[0], dims, preferred_element_type=F32)
    total += lax.dot_general(left[0], right[1], dims, preferred_element_type=F32)
    return total + lax.dot_general(left[1], right[0], dims, preferred_element_type=F32)


def panel_kernel(tile, inverse, out):
    inv = halves(inverse[...])
    for c in range(4):
        block = tile[pl.ds(c, NB, stride=4), :]
        out[128 * c : 128 * c + 128] = dot3(halves(block.T), inv, NT)


def where_am_i():
    return [lax.axis_index(axis) for axis in AXES]


def position(place, dx, dz):
    y, c, z = place[0], place[1], place[3]
    zt = (z + dz) % 8
    return pl.multiple_of((((zt + c) % 2) * 4 + (zt // 2 - y + 4) % 4) * 64 + dx * 16, 16)


def solve_kernel(tile, inverse, cols, *rest):
    panel = rest[:4]
    early = rest[4:12]
    late = rest[12:20]
    schur, kept, sent, own = rest[20:24]
    rows, sides, qh, ql, first, fh, fl, ch, sem_p, sem_e, sem_l = rest[24:]
    place = where_am_i()
    x = place[2]
    now = pl.program_id(0)
    nrow = tile.shape[0] // 4
    count = nrow // NB
    is_top = jnp.logical_and(place[0] * 2 + place[1] == 0, now == 0)
    copies, fetch = [], []
    for dx in range(4):
        xt = (x + dx) % 4
        for b in range(2):
            row = pl.multiple_of((4 * b + xt) * NB, NB)
            source = panel[dx].at[pl.ds(NB * b, NB)]
            copies.append(pltpu.make_async_copy(source, rows.at[pl.ds(row, NB)], sem_p.at[2 * dx + b]))
    for refs, low, size, sem in ((late, CUT, 9 - CUT, sem_l), (early, 0, CUT, sem_e)):
        for dz in range(8):
            fetch.append(pltpu.make_async_copy(refs[dz], sides.at[dz, :, pl.ds(low, size)], sem.at[dz]))

    @pl.when(now == 0)
    def _():
        for copy in copies + fetch:
            copy.start()
        high, low = halves(cols[...])
        qh[...] = high
        ql[...] = low
        for copy in copies:
            copy.wait()

    @pl.when(now == 0)
    def _():
        for copy in fetch:
            copy.wait()
        for dx in range(4):
            for dz in range(8):
                first[pl.ds(position(place, dx, dz), 16), :] = sides[dz, dx, 8]
        value = dot3(halves(first[...]), halves(inverse[...]), NT)
        first[...] = value
        high, low = halves(value)
        fh[...] = high
        fl[...] = low

    start = pl.multiple_of(now * nrow, nrow)
    mine = halves(rows[pl.ds(start, nrow), :])
    ch[...] = dot3((fh[...], fl[...]), mine, NT)
    for dx in range(4):
        for dz in range(8):
            row = position(place, dx, dz)
            for j in range(count):
                spot = (pl.ds(row, 16), slice(j * NB, j * NB + NB))
                value = sides[dz, dx, now * count + j] - ch[spot]
                if j == 0:
                    value = jnp.where(is_top, first[pl.ds(row, 16), :], value)
                if dx == 0 and dz == 0:
                    own[now * count + j] = value
                ch[spot] = value
    delta = dot3(mine, (qh[...], ql[...]), NT)
    pieces = []
    for c in range(4):
        value = tile[pl.ds(c, nrow, stride=4), :] - delta[:, 128 * c : 128 * c + 128]
        schur[pl.ds(c, nrow, stride=4), :] = value
        pieces.append(value)
    right = halves(jnp.concatenate(pieces, axis=1))

    left = halves(ch[...])
    upper = dot3((left[0][:256], left[1][:256]), right, NN)
    lower = dot3((left[0][256:], left[1][256:]), right, NN)

    @pl.when(now == 0)
    def _():
        kept[...] = upper
        sent[...] = lower

    @pl.when(now > 0)
    def _():
        kept[...] += upper
        sent[...] += lower


def finish_kernel(shifts, own, r0, r1, r2, r3, out):
    x = lax.axis_index("x")
    scale = shifts[x]
    for dx, ref in enumerate((r0, r1, r2, r3)):
        for b in range(2):
            a = 4 * b + (x - dx + 4) % 4
            out[a] = ref[:, b * NB : b * NB + NB] + own[a] * scale


def vmem():
    return pl.BlockSpec(memory_space=pltpu.VMEM)


def smem():
    return pl.BlockSpec(memory_space=pltpu.SMEM)


def step(array, axis, by):
    size = lax.axis_size(axis)
    return lax.ppermute(array, axis, [(i, (i + by) % size) for i in range(size)])


def x_then_z(block, last):
    line = jnp.stack([block, step(block, "x", -1), step(block, "x", 2), step(block, "x", 1)])
    got = {0: line}
    for r in (1, 2, 3):
        got[r] = step(got[r - 1], "z", -1)
        got[8 - r] = step(got[(9 - r) % 8], "z", 1)
    got[4] = step(got[3], "z", -1) if last > 0 else step(got[5], "z", 1)
    return [got[d] for d in range(8)]


def index(y, c, x, z):
    return ((y * NC + c) * NX + x) * NZ + z


def to_everyone_in_row(array):
    y, c = lax.axis_index("y"), lax.axis_index("c")
    got = lax.ppermute(array, ("y", "c"), [(0, 4)])
    array = jnp.where(y == 2, got, array)
    got = lax.ppermute(array, ("y", "c"), [(0, 2), (4, 6)])
    array = jnp.where(y % 2 == 1, got, array)
    got = lax.ppermute(array, "c", [(0, 1)])
    return jnp.where(c == 1, got, array)


def panel_rows(cols):
    axes = AXES
    c, z = lax.axis_index("c"), lax.axis_index("z")
    p = 2 * lax.axis_index("y") + c
    near, far, second, third = [], [], [], []
    for x in range(NX):
        for s in range(NZ):
            y, core = s // 2, s % 2
            near.append((index(0, 0, x, s), index(y, core, x, s)))
            far.append((index(0, 0, x, s), index(y, core, x, (s + 4) % 8)))
            for k in (0, 4):
                by = 2 if core == 0 else -2
                second.append((index(y, core, x, (s + k) % 8), index(y, core, x, (s + k + by) % 8)))
            for k in (0, 2, 4, 6):
                third.append((index(y, core, x, (s + k) % 8), index(y, core, x, (s + k + 1) % 8)))
    offset = (z - p + 8) % 8

    def move(array, pairs):
        return lax.ppermute(array, axes, pairs)

    block = jnp.where(offset == 0, move(cols, near), move(cols, far))
    block = jnp.where(offset % 4 == 0, block, move(block, second))
    block = jnp.where(offset % 2 == 0, block, move(block, third))
    right = step(block, "x", -1)
    left = step(block, "x", 1)
    pairs = []
    for y in range(NY):
        for core in range(NC):
            by = -1 if core == 0 else 1
            for x in range(NX):
                for s in range(NZ):
                    pairs.append((index(y, core, x, s), index(y, core, (x + by) % NX, s)))
    across = move(jnp.where(c == 0, right, left), pairs)
    return block, right, across, left


def shards(normal, panel_inverse, rhs, shifts):
    axes = AXES
    tile = normal.reshape(8192, 128)
    right = jnp.transpose(rhs.reshape(8, NB, 16), (0, 2, 1))
    early = x_then_z(right[:CUT], 1)
    top = to_everyone_in_row(right[0])
    late = x_then_z(jnp.concatenate([right[CUT:], top[None]], axis=0), -1)

    cols = pl.pallas_call(
        panel_kernel,
        grid=(1,),
        in_specs=[pl.BlockSpec((1024, 128), lambda i: (0, 0)), pl.BlockSpec((NB, NB), lambda i: (0, 0))],
        out_specs=pl.BlockSpec((512, NB), lambda i: (0, 0)),
        out_shape=jax.ShapeDtypeStruct((512, NB), F32),
        name="panel",
    )(tile, panel_inverse)
    panel = panel_rows(cols)
    cols = to_everyone_in_row(cols)

    nrow = 1024
    whole = lambda shape: pl.BlockSpec(shape, lambda i: (0,) * len(shape))
    remote = pl.BlockSpec(memory_space=pl.ANY)
    schur, kept, sent, own = pl.pallas_call(
        solve_kernel,
        grid=(2048 // nrow,),
        in_specs=[pl.BlockSpec((nrow * 4, 128), lambda i: (i, 0)), whole((NB, NB)), whole((512, NB))]
        + [remote] * 20,
        out_specs=[
            pl.BlockSpec((nrow * 4, 128), lambda i: (i, 0)),
            whole((256, 512)),
            whole((256, 512)),
            whole((8, 16, NB)),
        ],
        out_shape=[
            jax.ShapeDtypeStruct((8192, 128), F32),
            jax.ShapeDtypeStruct((256, 512), F32),
            jax.ShapeDtypeStruct((256, 512), F32),
            jax.ShapeDtypeStruct((8, 16, NB), F32),
        ],
        scratch_shapes=[
            pltpu.VMEM((2048, NB), F32),
            pltpu.VMEM((8, 4, 9, 16, NB), F32),
            pltpu.VMEM((512, NB), BF16),
            pltpu.VMEM((512, NB), BF16),
            pltpu.VMEM((512, NB), F32),
            pltpu.VMEM((512, NB), BF16),
            pltpu.VMEM((512, NB), BF16),
            pltpu.VMEM((512, nrow), F32),
            pltpu.SemaphoreType.DMA((8,)),
            pltpu.SemaphoreType.DMA((8,)),
            pltpu.SemaphoreType.DMA((8,)),
        ],
        name="solve",
    )(tile, panel_inverse, cols, *panel, *early, *late)

    kept = kept + lax.ppermute(sent, "c", [(0, 1), (1, 0)])
    parts = [step(kept[64 * r : 64 * r + 64], "y", r) for r in (1, 2, 3)]
    total = kept[:64] + parts[0] + parts[1] + parts[2]
    pairs = [
        (index(p // 2, p % 2, x, z), index(z // 2, z % 2, x, p))
        for p in range(8)
        for x in range(NX)
        for z in range(NZ)
    ]
    total = lax.ppermute(total, axes, pairs)
    arrived = [total[:16]] + [step(total[16 * dx : 16 * dx + 16], "x", dx) for dx in (1, 2, 3)]
    applied = pl.pallas_call(
        finish_kernel,
        in_specs=[smem()] + [vmem()] * 5,
        out_specs=vmem(),
        out_shape=jax.ShapeDtypeStruct((8, 16, NB), F32),
        name="finish",
    )(shifts, own, *arrived)

    def in_rhs_layout(array):
        return jnp.transpose(array, (0, 2, 1)).reshape(8, 1, NB, 16)

    return schur.reshape(8, 1, NB, 2, 1, NB), in_rhs_layout(own), in_rhs_layout(applied)


def solution(mesh):
    split = Mesh(mesh.devices.reshape(NY, NC, NX, NZ), AXES)
    row, col = ("y", "c"), ("x", "z")
    matrix = P(None, row, None, None, col, None)
    sides = P(None, row, None, col)
    return jax.shard_map(
        shards,
        mesh=split,
        in_specs=(matrix, P(), sides, P()),
        out_specs=(matrix, sides, sides),
        check_vma=False,
    )
```
